8 devices in a mesh: rep: 2 (over y, z), dp: 4 (over x, core).
Axes of the slice: x: 2, y: 2, z: 1, core: 2. Of those that a mesh axis runs over, the one named last changes fastest.
Arguments:
- x: bfloat16 [8, 2048, 768], P(('rep', 'dp')), parts along dimension 0
- dy: bfloat16 [8, 2048, 768], P(('rep', 'dp')), parts along dimension 0
- wq: bfloat16 [2, 768, 768], P(None, 'dp')
- wk: bfloat16 [2, 768, 128], P(None, 'dp')
- wv: bfloat16 [2, 768, 128], P(None, 'dp')
- wo: bfloat16 [2, 768, 768], P(None, 'dp')
- w_gate: bfloat16 [2, 768, 2048], P(None, 'dp')
- w_up: bfloat16 [2, 768, 2048], P(None, 'dp')
- w_down: bfloat16 [2, 2048, 768], P(None, 'dp')
- m_wq: float32 [2, 768, 768], P(None, 'dp')
- m_wk: float32 [2, 768, 128], P(None, 'dp')
- m_wv: float32 [2, 768, 128], P(None, 'dp')
- m_wo: float32 [2, 768, 768], P(None, 'dp')
- m_w_gate: float32 [2, 768, 2048], P(None, 'dp')
- m_w_up: float32 [2, 768, 2048], P(None, 'dp')
- m_w_down: float32 [2, 2048, 768], P(None, 'dp')
- v_wq: float32 [2, 768, 768], P(None, 'dp')
- v_wk: float32 [2, 768, 128], P(None, 'dp')
- v_wv: float32 [2, 768, 128], P(None, 'dp')
- v_wo: float32 [2, 768, 768], P(None, 'dp')
- v_w_gate: float32 [2, 768, 2048], P(None, 'dp')
- v_w_up: float32 [2, 768, 2048], P(None, 'dp')
- v_w_down: float32 [2, 2048, 768], P(None, 'dp')
Outputs:
- output 1: bfloat16 [4, 768, 768], P('rep', 'dp'), parts along dimension 0
- output 2: bfloat16 [4, 768, 128], P('rep', 'dp'), parts along dimension 0
- output 3: bfloat16 [4, 768, 128], P('rep', 'dp'), parts along dimension 0
- output 4: bfloat16 [4, 768, 768], P('rep', 'dp'), parts along dimension 0
- output 5: bfloat16 [4, 768, 2048], P('rep', 'dp'), parts along dimension 0
- output 6: bfloat16 [4, 768, 2048], P('rep', 'dp'), parts along dimension 0
- output 7: bfloat16 [4, 2048, 768], P('rep', 'dp'), parts along dimension 0
- output 8: float32 [4, 768, 768], P('rep', 'dp'), parts along dimension 0
- output 9: float32 [4, 768, 128], P('rep', 'dp'), parts along dimension 0
- output 10: float32 [4, 768, 128], P('rep', 'dp'), parts along dimension 0
- output 11: float32 [4, 768, 768], P('rep', 'dp'), parts along dimension 0
- output 12: float32 [4, 768, 2048], P('rep', 'dp'), parts along dimension 0
- output 13: float32 [4, 768, 2048], P('rep', 'dp'), parts along dimension 0
- output 14: float32 [4, 2048, 768], P('rep', 'dp'), parts along dimension 0
- output 15: float32 [4, 768, 768], P('rep', 'dp'), parts along dimension 0
- output 16: float32 [4, 768, 128], P('rep', 'dp'), parts along dimension 0
- output 17: float32 [4, 768, 128], P('rep', 'dp'), parts along dimension 0
- output 18: float32 [4, 768, 768], P('rep', 'dp'), parts along dimension 0
- output 19: float32 [4, 768, 2048], P('rep', 'dp'), parts along dimension 0
- output 20: float32 [4, 768, 2048], P('rep', 'dp'), parts along dimension 0
- output 21: float32 [4, 2048, 768], P('rep', 'dp'), parts along dimension 0
There are 2 independent parts. The reference program is written for one: setup_inputs(seed, part) draws one part's arguments, and reference() takes and returns one part's arrays. A program takes and returns all parts, laid end to end along the dimension named above; an argument that names none is the same for every part.
All inputs are finite; a program needn't handle non-finite values.
Results may differ from the reference program's by a relative error of at most 0.0279.
Values are sent between devices in bfloat16 or wider.
A program may use at most 2 GiB of HBM per device.

```python
import jax
import jax.numpy as jnp
from jax import lax

SEQUENCES = 4
TOKENS = 2048
D = 768
HEADS = 6
KV_HEADS = 1
HEAD = 128
FF = 2048
LAYERS = 2
THETA = 10000
NAMES = ("wq", "wk", "wv", "wo", "w_gate", "w_up", "w_down")
SHAPES = {
    "wq": (LAYERS, D, HEADS * HEAD),
    "wk": (LAYERS, D, KV_HEADS * HEAD),
    "wv": (LAYERS, D, KV_HEADS * HEAD),
    "wo": (LAYERS, HEADS * HEAD, D),
    "w_gate": (LAYERS, D, FF),
    "w_up": (LAYERS, D, FF),
    "w_down": (LAYERS, FF, D),
}


def bump(key, n, height):
    away = (jnp.arange(n, dtype=jnp.int32) - jax.random.randint(key, (), 0, n, jnp.int32)) % n
    return jnp.where(away < n // 8, height, 1.0)


def together(key, own, strength):
    shared = jax.random.normal(key, own.shape[1:], jnp.float32)
    return (own + strength * shared) * lax.rsqrt(1 + strength * strength)


def setup_inputs(seed: int = 0, part: int = 0) -> dict:
    kx, kdy, ka, kb, kz, kf, kh, kl, *keys = jax.random.split(jax.random.key(seed), 8 + 3 * len(NAMES))
    kx, kdy, ka, kb = (jax.random.fold_in(k, part) for k in (kx, kdy, ka, kb))
    kw, km, kv = (keys[i::3] for i in range(3))
    shape = (SEQUENCES, TOKENS, D)
    much_x, much_dy = jax.random.uniform(kz, (2,), jnp.float32, 0.0, 1.0)
    loud = 2.0 ** jax.random.uniform(jax.random.fold_in(kz, 1), (), jnp.float32, -1.0, 2.0)
    layers = 2.0 ** jax.random.uniform(kl, (LAYERS, 1, 1), jnp.float32, -1.0, 1.0)
    times = {"wq": 1.0, "wk": 1.0, "wv": 2.0, "wo": layers, "w_gate": 1.0, "w_up": bump(kh, FF, 4.0), "w_down": layers}
    x = together(ka, jax.random.normal(kx, shape, jnp.float32), much_x) * bump(kf, D, 4.0)
    dy = together(kb, jax.random.normal(kdy, shape, jnp.float32), much_dy)
    drawn = {"x": x.astype(jnp.bfloat16), "dy": (loud * dy * (SEQUENCES * TOKENS) ** -0.5).astype(jnp.bfloat16)}
    for key, name in zip(kw, NAMES, strict=True):
        drawn[name] = (jax.random.normal(key, SHAPES[name], jnp.float32) * SHAPES[name][1] ** -0.5 * times[name]).astype(jnp.bfloat16)
    for key, name in zip(km, NAMES, strict=True):
        drawn[f"m_{name}"] = 0.1 * jax.random.normal(key, SHAPES[name], jnp.float32)
    for key, name in zip(kv, NAMES, strict=True):
        drawn[f"v_{name}"] = jax.random.uniform(key, SHAPES[name], jnp.float32, 0.02, 0.06)
    return drawn


def matmul(a, w):
    return jnp.dot(a, w, preferred_element_type=jnp.float32).astype(jnp.bfloat16)


def normed(h):
    wide = h.astype(jnp.float32)
    scale = lax.rsqrt(jnp.mean(wide**2, -1, keepdims=True) + 1e-6)
    return (wide * scale).astype(jnp.bfloat16)


def turned(t, theta):
    half = t.shape[-1] // 2
    angle = jnp.arange(t.shape[0], dtype=jnp.float32)[:, None] * theta ** (-jnp.arange(half, dtype=jnp.float32) / half)
    cos, sin = jnp.cos(angle)[:, None], jnp.sin(angle)[:, None]
    a, b = t[..., :half].astype(jnp.float32), t[..., half:].astype(jnp.float32)
    return jnp.concatenate([a * cos - b * sin, b * cos + a * sin], -1).astype(jnp.bfloat16)


def seen_by(q, k, v):
    tokens, kv = q.shape[0], k.shape[1]
    q = q.reshape(tokens, kv, -1, q.shape[-1])
    scores = jnp.einsum("tgsd,ugd->gstu", q.astype(jnp.float32), k.astype(jnp.float32)) * q.shape[-1] ** -0.5
    place = jnp.arange(tokens)
    weights = jax.nn.softmax(jnp.where(place[:, None] >= place, scores, -jnp.inf), -1).astype(jnp.bfloat16)
    return jnp.einsum("gstu,ugd->tgsd", weights.astype(jnp.float32), v.astype(jnp.float32)).astype(jnp.bfloat16).reshape(tokens, -1)


def layer(h, w):
    a = normed(h)
    q, k = (turned(matmul(a, w[name]).reshape(h.shape[0], -1, HEAD), THETA) for name in ("wq", "wk"))
    h = h + matmul(seen_by(q, k, matmul(a, w["wv"]).reshape(h.shape[0], -1, HEAD)), w["wo"])
    b = normed(h)
    gate = jnp.dot(b, w["w_gate"], preferred_element_type=jnp.float32)
    up = jnp.dot(b, w["w_up"], preferred_element_type=jnp.float32)
    return h + matmul((jax.nn.silu(gate) * up).astype(jnp.bfloat16), w["w_down"])


def adamw(w, m, v, g):
    m = 0.9 * m + 0.1 * g
    v = 0.95 * v + 0.05 * g * g
    step = m * lax.rsqrt(v + 1e-8) + 0.1 * w
    return (w - 0.02 * step).astype(jnp.bfloat16), m, v


def clipped(gradients, sum_of_squares, count):
    factor = jnp.minimum(1.0, 0.5 * lax.rsqrt(sum_of_squares / count + 1e-30))
    return [g * factor for g in gradients]


def stack(weights, h):
    return lax.scan(lambda h, w: (layer(h, w), None), h, weights)[0]


def reference(x, dy, wq, wk, wv, wo, w_gate, w_up, w_down, m_wq, m_wk, m_wv, m_wo, m_w_gate, m_w_up, m_w_down, v_wq, v_wk, v_wv, v_wo, v_w_gate, v_w_up, v_w_down):
    weights = dict(zip(NAMES, (wq, wk, wv, wo, w_gate, w_up, w_down), strict=True))

    def take(so_far, sequence):
        h, by_y = sequence
        _, back = jax.vjp(stack, weights, h)
        by_weights, by_h = back(by_y)
        return jax.tree.map(lambda total, term: total + term.astype(jnp.float32), so_far, by_weights), by_h

    none_yet = {name: jnp.zeros(w.shape, jnp.float32) for name, w in weights.items()}
    by_weights, by_x = lax.scan(take, none_yet, (x, dy))
    gradients = [by_weights[name].astype(jnp.bfloat16).astype(jnp.float32) for name in NAMES]
    gradients = clipped(gradients, sum(jnp.sum(g * g) for g in gradients), sum(g.size for g in gradients))
    first = (m_wq, m_wk, m_wv, m_wo, m_w_gate, m_w_up, m_w_down)
    second = (v_wq, v_wk, v_wv, v_wo, v_w_gate, v_w_up, v_w_down)
    new = [adamw(weights[name].astype(jnp.float32), m, v, g) for name, m, v, g in zip(NAMES, first, second, gradients, strict=True)]
    return tuple(one[which] for which in range(3) for one in new)
```

```python
import functools

import jax
import jax.numpy as jnp
from jax import lax
from jax.experimental import pallas as pl
from jax.experimental.pallas import tpu as pltpu
from jax.sharding import PartitionSpec as P

NEG = -1e30
HIDDEN = 2 * NEG
LOG2E = 1.4426950408889634
HEAD = 128
THETA = 10000
VMEM = 62 * 2**20
TILE = 512
F32, BF16 = jnp.float32, jnp.bfloat16
ANY = pl.BlockSpec(memory_space=pl.ANY)


def _dot(a, b, ca=1, cb=0):
    return lax.dot_general(a, b, (((ca,), (cb,)), ((), ())), preferred_element_type=F32)


def _scale(h):
    return lax.rsqrt(jnp.mean(h * h, -1, keepdims=True) + 1e-6)


def _norm(h):
    h = h.astype(F32)
    return (h * _scale(h)).astype(BF16)


def _norm_back(h, d):
    h = h.astype(F32)
    r = _scale(h)
    n = h * r
    return r * (d - n * jnp.mean(d * n, -1, keepdims=True))


def _turn(t, cos, sin):
    return t * cos + pltpu.roll(t, HEAD // 2, 1) * sin


def _copies(pieces, dst, rows, me, sem, at=0, width=None):
    rep, dp = me
    own, px, py, cown, cpx, cpy = pieces
    half = rows // 2
    starts = [dp * rows, (dp ^ 2) * rows + rep * half, (dp ^ 2) * rows + (1 - rep) * half, (dp ^ 1) * rows,
              (dp ^ 3) * rows + rep * half, (dp ^ 3) * rows + (1 - rep) * half]
    out = []
    for piece, start, size in zip((own, px, py, cown, cpx, cpy), starts, (rows, half, half, rows, half, half)):
        src = piece if width is None else piece.at[:, pl.ds(at, width)]
        out.append(pltpu.make_async_copy(src, dst.at[pl.ds(pl.multiple_of(start, half), size), :], sem))
    return out


def _attend_kernel(me_ref, h_ref, cos_ref, sin_ref, *rest, tokens, heads):
    w, rest = rest[:6], rest[6:]
    q_ref, k_ref, v_ref, o_ref, lse_ref, w_s, k_s, v_s, top_s, mix_s, sem = rest
    iq = pl.program_id(0)
    d = heads * HEAD
    e = HEAD**-0.5 * LOG2E

    @pl.when(iq == 0)
    def _():
        todo = _copies(w, w_s, w_s.shape[0] // 4, (me_ref[0], me_ref[1]), sem)
        for c in todo:
            c.start()
        for c in todo:
            c.wait()
        v_s[HEAD:, :] = jnp.ones((8, tokens), BF16)

    y = _dot(_norm(h_ref[...]), w_s[...]).astype(BF16)
    cos, sin = cos_ref[...], sin_ref[...]
    for n in range(heads):
        q_ref[:, n * HEAD : (n + 1) * HEAD] = _turn(y[:, n * HEAD : (n + 1) * HEAD].astype(F32), cos, sin).astype(BF16)
    k = _turn(y[:, d : d + HEAD].astype(F32), cos, sin).astype(BF16)
    v = y[:, d + HEAD :]
    k_ref[...] = k
    v_ref[...] = v
    here = pl.ds(pl.multiple_of(iq * TILE, TILE), TILE)
    k_s[here, :] = k
    v_s[:HEAD, here] = v.T
    top_s[...] = jnp.full(top_s.shape, NEG, F32)
    mix_s[...] = jnp.zeros(mix_s.shape, F32)

    def block(start, size, first, masked):
        keys = pl.ds(pl.multiple_of(start, 256), size)
        width = TILE - first
        scores = [_dot(k_s[keys, :], q_ref[first:, n * HEAD : (n + 1) * HEAD], 1, 1) for n in range(heads)]
        if masked:
            ok = lax.broadcasted_iota(jnp.int32, (size, width), 1) >= lax.broadcasted_iota(jnp.int32, (size, width), 0)
        weights, keeps = [], []
        for n, s in enumerate(scores):
            if masked:
                s = jnp.where(ok, s, HIDDEN)
            old = top_s[n : n + 1, first:]
            top = jnp.maximum(old, s.max(axis=0, keepdims=True))
            top_s[n : n + 1, first:] = top
            weights.append(jnp.exp2((s - top) * e).astype(BF16))
            keeps.append(jnp.exp2((old - top) * e))
        for n, (p, keep) in enumerate(zip(weights, keeps)):
            mix_s[n, :, first:] = mix_s[n, :, first:] * keep + _dot(v_s[:, keys], p)

    lax.fori_loop(0, iq, lambda j, _: block(j * TILE, TILE, 0, False), None)
    block(iq * TILE, 256, 0, True)
    block(iq * TILE + 256, 256, 256, True)
    for n in range(heads):
        total = mix_s[n, HEAD : HEAD + 1, :]
        o_ref[:, n * HEAD : (n + 1) * HEAD] = (mix_s[n, :HEAD, :] * (1 / total)).T.astype(BF16)
        lse_ref[n : n + 1, :] = top_s[n : n + 1, :] * e + jnp.log2(total)


def attend(me, h, cos, sin, w):
    tokens, d = h.shape
    heads = d // HEAD
    rows = lambda n: pl.BlockSpec((TILE, n), lambda i, _: (i, 0))
    flops = 2 * tokens * d * (d + 2 * HEAD) + 3 * 2 * heads * tokens * tokens * HEAD
    return pl.pallas_call(
        functools.partial(_attend_kernel, tokens=tokens, heads=heads),
        name="attend",
        grid_spec=pltpu.PrefetchScalarGridSpec(
            num_scalar_prefetch=1,
            grid=(tokens // TILE,),
            in_specs=[rows(d), rows(HEAD), rows(HEAD)] + [ANY] * 6,
            out_specs=[rows(d), rows(HEAD), rows(HEAD), rows(d), pl.BlockSpec((heads, TILE), lambda i, _: (0, i))],
            scratch_shapes=[pltpu.VMEM((d, d + 2 * HEAD), BF16), pltpu.VMEM((tokens, HEAD), BF16), pltpu.VMEM((HEAD + 8, tokens), BF16),
                            pltpu.VMEM((8, TILE), F32), pltpu.VMEM((heads, HEAD + 8, TILE), F32), pltpu.SemaphoreType.DMA],
        ),
        out_shape=[jax.ShapeDtypeStruct((tokens, d), BF16), jax.ShapeDtypeStruct((tokens, HEAD), BF16), jax.ShapeDtypeStruct((tokens, HEAD), BF16),
                   jax.ShapeDtypeStruct((tokens, d), BF16), jax.ShapeDtypeStruct((heads, tokens), F32)],
        compiler_params=pltpu.CompilerParams(dimension_semantics=("arbitrary",), vmem_limit_bytes=VMEM),
        cost_estimate=pl.CostEstimate(flops=flops, transcendentals=heads * tokens * tokens // 2, bytes_accessed=10 * tokens * d),
    )(me, h, cos, sin, *w)


def _forward_kernel(me_ref, h_ref, o_ref, *rest, ff):
    wo, wgu, wd, rest = rest[:6], rest[6:12], rest[12:18], rest[18:]
    h1_ref, h2_ref, wo_s, wg_s, wu_s, wd_s, act_s, sem = rest
    first = pl.program_id(0) == 0
    me = (me_ref[0], me_ref[1])
    d = wo_s.shape[0]
    loads = (lambda: _copies(wo, wo_s, d // 4, me, sem.at[0]),
             lambda: _copies(wgu, wg_s, d // 4, me, sem.at[1], 0, ff) + _copies(wgu, wu_s, d // 4, me, sem.at[1], ff, ff),
             lambda: _copies(wd, wd_s, ff // 4, me, sem.at[2]))

    @pl.when(first)
    def _():
        for group in loads:
            for c in group():
                c.start()
        for c in loads[0]():
            c.wait()

    proj = _dot(o_ref[...], wo_s[...]).astype(BF16)
    h1 = (h_ref[...].astype(F32) + proj.astype(F32)).astype(BF16)
    h1_ref[...] = h1
    b = _norm(h1)

    @pl.when(first)
    def _():
        for group in loads[1:]:
            for c in group():
                c.wait()

    for at in range(0, ff, TILE):
        g = _dot(b, wg_s[:, at : at + TILE])
        u = _dot(b, wu_s[:, at : at + TILE])
        act_s[:, at : at + TILE] = (g * (1 / (1 + jnp.exp(-g))) * u).astype(BF16)
    y = _dot(act_s[...], wd_s[...]).astype(BF16)
    h2_ref[...] = (h1.astype(F32) + y.astype(F32)).astype(BF16)


def forward(me, h, o, wo, wgu, wd):
    tokens, d = h.shape
    ff = wgu[0].shape[1] // 2
    rows = pl.BlockSpec((TILE, d), lambda i, _: (i, 0))
    return pl.pallas_call(
        functools.partial(_forward_kernel, ff=ff),
        name="forward",
        grid_spec=pltpu.PrefetchScalarGridSpec(
            num_scalar_prefetch=1,
            grid=(tokens // TILE,),
            in_specs=[rows, rows] + [ANY] * 18,
            out_specs=[rows, rows],
            scratch_shapes=[pltpu.VMEM((d, d), BF16), pltpu.VMEM((d, ff), BF16), pltpu.VMEM((d, ff), BF16), pltpu.VMEM((ff, d), BF16),
                            pltpu.VMEM((TILE, ff), BF16), pltpu.SemaphoreType.DMA((3,))],
        ),
        out_shape=[jax.ShapeDtypeStruct((tokens, d), BF16)] * 2,
        compiler_params=pltpu.CompilerParams(dimension_semantics=("arbitrary",), vmem_limit_bytes=VMEM),
        cost_estimate=pl.CostEstimate(flops=2 * tokens * d * (d + 3 * ff), transcendentals=tokens * ff, bytes_accessed=8 * tokens * d + 2 * d * (d + 3 * ff)),
    )(me, h, o, *wo, *wgu, *wd)


def _ff_back_kernel(me_ref, h_ref, o_ref, dy_ref, *rest, ff, project):
    wo, rest = (rest[:6], rest[6:]) if project else (None, rest)
    wgu, wd, rest = rest[:6], rest[6:12], rest[12:]
    dh_ref, h1_ref, gu_keep, gu_send, d_keep, d_send, o_keep, o_send = (rest[:1] + rest[1:2] + rest[2:8]) if project else (rest[:1] + (None,) + rest[1:7])
    scratch = rest[8:] if project else rest[7:]
    wo_s, scratch = (scratch[0], scratch[1:]) if project else (None, scratch)
    wg_s, wu_s, wd_s, b_s, t_s, db_s, act_s, dg_s, du_s, sem = scratch
    step = pl.program_id(0)
    me = (me_ref[0], me_ref[1])
    tokens, d = h_ref.shape
    rows = d // 4
    h1 = h1_ref if project else h_ref
    loads = (lambda: _copies(wo, wo_s, rows, me, sem.at[0]) if project else [],
             lambda: _copies(wgu, wg_s, rows, me, sem.at[1], 0, ff) + _copies(wgu, wu_s, rows, me, sem.at[1], ff, ff),
             lambda: _copies(wd, wd_s, ff // 4, me, sem.at[2]))

    def transposed(value, at):
        for n in range(4):
            to = pl.multiple_of((me[1] ^ n) * rows, rows)
            t_s[pl.ds(to, rows), at : at + TILE] = value[:, n * rows : (n + 1) * rows].T

    @pl.when(step == 0)
    def _():
        for group in loads:
            for c in group():
                c.start()
        for c in loads[0]():
            c.wait()
        for at in range(0, tokens, TILE):
            here = slice(at, at + TILE)
            h = h_ref[here, :]
            if project:
                h = (h.astype(F32) + _dot(o_ref[here, :], wo_s[...]).astype(BF16).astype(F32)).astype(BF16)
                h1_ref[here, :] = h
            b = _norm(h)
            b_s[here, :] = b
            transposed(b, at)
        db_s[...] = jnp.zeros(db_s.shape, F32)
        for group in loads[1:]:
            for c in group():
                c.wait()

    tile = me[1] ^ step
    cols = pl.ds(pl.multiple_of(tile * TILE, TILE), TILE)
    for at in range(0, tokens, TILE):
        here = slice(at, at + TILE)
        b = b_s[here, :]
        g = _dot(b, wg_s[:, cols])
        u = _dot(b, wu_s[:, cols])
        da = _dot(dy_ref[here, :], wd_s[cols, :], 1, 1).astype(BF16).astype(F32)
        sig = 1 / (1 + jnp.exp(-g))
        silu = g * sig
        act_s[here, :] = (silu * u).astype(BF16)
        dg = (da * u * (sig * (1 + g * (1 - sig)))).astype(BF16)
        du = (da * silu).astype(BF16)
        dg_s[here, :] = dg
        du_s[here, :] = du
        db_s[here, :] += _dot(dg, wg_s[:, cols], 1, 1) + _dot(du, wu_s[:, cols], 1, 1)
    for n, part in enumerate((dg_s, du_s)):
        grad = _dot(t_s[...], part[...]).astype(BF16)
        for j, to in enumerate((gu_keep, gu_send, gu_keep, gu_send)):
            to[j // 2, n] = grad[j * rows : (j + 1) * rows, :]
    grad = _dot(act_s[...], dy_ref[...], 0, 0).astype(BF16)

    @pl.when(step % 2 == 0)
    def _():
        d_keep[0] = grad

    @pl.when(step % 2 == 1)
    def _():
        d_send[0] = grad

    @pl.when(step == 3)
    def _():
        for at in range(0, tokens, TILE):
            here = slice(at, at + TILE)
            db = db_s[here, :].astype(BF16).astype(F32)
            dh_ref[here, :] = (dy_ref[here, :].astype(F32) + _norm_back(h1[here, :], db).astype(BF16).astype(F32)).astype(BF16)
            transposed(o_ref[here, :], at)
        grad = _dot(t_s[...], dh_ref[...]).astype(BF16)
        for j, to in enumerate((o_keep, o_send, o_keep, o_send)):
            to[j // 2] = grad[j * rows : (j + 1) * rows, :]


def ff_back(me, h, o, dy, wo, wgu, wd, project):
    tokens, d = h.shape
    ff = wgu[0].shape[1] // 2
    once = pl.Buffered(1)
    whole = lambda *shape: pl.BlockSpec(shape, lambda i, _: (0,) * len(shape), pipeline_mode=once)
    gu = pl.BlockSpec((2, 2, d // 4, TILE), lambda i, me: (0, 0, 0, me[1] ^ i))
    down = pl.BlockSpec((1, TILE, d), lambda i, _: (i // 2, 0, 0))
    states = jax.ShapeDtypeStruct((tokens, d), BF16)
    gu_shape = jax.ShapeDtypeStruct((2, 2, d // 4, ff), BF16)
    down_shape = jax.ShapeDtypeStruct((2, ff // 4, d), BF16)
    o_shape = jax.ShapeDtypeStruct((2, d // 4, d), BF16)
    n_states = 2 if project else 1
    n_w = 18 if project else 12
    out = pl.pallas_call(
        functools.partial(_ff_back_kernel, ff=ff, project=project),
        name="ff_back",
        grid_spec=pltpu.PrefetchScalarGridSpec(
            num_scalar_prefetch=1,
            grid=(4,),
            in_specs=[whole(tokens, d)] * 3 + [ANY] * n_w,
            out_specs=[whole(tokens, d)] * n_states + [gu, gu, down, down, whole(2, d // 4, d), whole(2, d // 4, d)],
            scratch_shapes=([pltpu.VMEM((d, d), BF16)] if project else [])
            + [pltpu.VMEM((d, ff), BF16), pltpu.VMEM((d, ff), BF16), pltpu.VMEM((ff, d), BF16), pltpu.VMEM((tokens, d), BF16),
               pltpu.VMEM((d, tokens), BF16), pltpu.VMEM((tokens, d), F32), pltpu.VMEM((tokens, TILE), BF16), pltpu.VMEM((tokens, TILE), BF16),
               pltpu.VMEM((tokens, TILE), BF16), pltpu.SemaphoreType.DMA((3,))],
        ),
        out_shape=[states] * n_states + [gu_shape, gu_shape, down_shape, down_shape, o_shape, o_shape],
        compiler_params=pltpu.CompilerParams(dimension_semantics=("arbitrary",), vmem_limit_bytes=VMEM),
        cost_estimate=pl.CostEstimate(flops=2 * tokens * d * (8 * ff + d * n_states), transcendentals=tokens * ff,
                                      bytes_accessed=10 * tokens * d + 12 * d * ff),
    )(me, h, o, dy, *((*wo,) if project else ()), *wgu, *wd)
    dh, h1 = (out[0], out[1]) if project else (out[0], h)
    gu_keep, gu_send, d_keep, d_send, o_keep, o_send = out[n_states:]
    return dh, h1, (gu_keep, gu_send), (d_keep, d_send), (o_keep, o_send)


def _attend_back_kernel(me_ref, h_ref, dh_ref, q_ref, o_ref, k_ref, v_ref, lse_ref, cos_ref, sin_ref, *rest, heads, tokens):
    wqkv, wo, rest = rest[:6], rest[6:12], rest[12:]
    out_ref, keep, send, w_s, wo_s, do_s, dq_s, dk_s, dv_s, dqkv_s, a_s, acc_s, delta_s, sem = rest
    step = pl.program_id(0)
    iq = tokens // TILE - 1 - step
    me = (me_ref[0], me_ref[1])
    d = heads * HEAD
    rows = d // 4
    scale = HEAD**-0.5
    e = scale * LOG2E

    @pl.when(step == 0)
    def _():
        todo = _copies(wqkv, w_s, rows, me, sem) + _copies(wo, wo_s, rows, me, sem)
        for c in todo:
            c.start()
        for c in todo:
            c.wait()
        dk_s[...] = jnp.zeros(dk_s.shape, F32)
        dv_s[...] = jnp.zeros(dv_s.shape, F32)
        acc_s[...] = jnp.zeros(acc_s.shape, F32)

    do_s[...] = _dot(dh_ref[...], wo_s[...], 1, 1).astype(BF16)
    for n in range(heads):
        at = slice(n * HEAD, (n + 1) * HEAD)
        delta_s[n : n + 1, :] = (do_s[:, at].astype(F32) * o_ref[:, at].astype(F32)).T.sum(axis=0, keepdims=True)
    dq_s[...] = jnp.zeros(dq_s.shape, F32)

    def block(start, size, first, masked):
        keys = pl.ds(pl.multiple_of(start, 256), size)
        width = TILE - first
        ats = [slice(n * HEAD, (n + 1) * HEAD) for n in range(heads)]
        k, v = k_ref[keys, :], v_ref[keys, :]
        scores = [_dot(k, q_ref[first:, at], 1, 1) for at in ats]
        dps = [_dot(v, do_s[first:, at], 1, 1) for at in ats]
        if masked:
            ok = lax.broadcasted_iota(jnp.int32, (size, width), 1) >= lax.broadcasted_iota(jnp.int32, (size, width), 0)
        for n, at in enumerate(ats):
            p = jnp.exp2(scores[n] * e - lse_ref[n : n + 1, first:])
            if masked:
                p = jnp.where(ok, p, 0.0)
            ds = (p * (dps[n] - delta_s[n : n + 1, first:])).astype(BF16)
            dv_s[keys, :] += _dot(p.astype(BF16), do_s[first:, at])
            dk_s[keys, :] += _dot(ds, q_ref[first:, at])
            dq_s[n, :, first:] += _dot(k.T, ds)

    lax.fori_loop(0, iq, lambda j, _: block(j * TILE, TILE, 0, False), None)
    block(iq * TILE, 256, 0, True)
    block(iq * TILE + 256, 256, 256, True)

    cos, sin = cos_ref[...], -sin_ref[...]
    for n in range(heads):
        dqkv_s[:, n * HEAD : (n + 1) * HEAD] = _turn((dq_s[n] * scale).T.astype(BF16).astype(F32), cos, sin).astype(BF16)
    here = pl.ds(pl.multiple_of(iq * TILE, TILE), TILE)
    dqkv_s[:, d : d + HEAD] = _turn((dk_s[here, :] * scale).astype(BF16).astype(F32), cos, sin).astype(BF16)
    dqkv_s[:, d + HEAD :] = dv_s[here, :].astype(BF16)
    da = _dot(dqkv_s[...], w_s[...], 1, 1).astype(BF16).astype(F32)
    out_ref[...] = (dh_ref[...].astype(F32) + _norm_back(h_ref[...], da).astype(BF16).astype(F32)).astype(BF16)
    a = _norm(h_ref[...])
    for n in range(4):
        to = pl.multiple_of((me[1] ^ n) * rows, rows)
        a_s[pl.ds(to, rows), :] = a[:, n * rows : (n + 1) * rows].T
    acc_s[...] += _dot(a_s[...], dqkv_s[...])

    @pl.when(step == tokens // TILE - 1)
    def _():
        for j, to in enumerate((keep, send, keep, send)):
            to[j // 2] = acc_s[j * rows : (j + 1) * rows, :].astype(BF16)


def attend_back(me, h, dh, q, o, k, v, lse, cos, sin, wqkv, wo):
    tokens, d = h.shape
    heads = d // HEAD
    last = tokens // TILE - 1
    once = pl.Buffered(1)
    rows = lambda n: pl.BlockSpec((TILE, n), lambda i, _: (last - i, 0))
    whole = lambda *shape: pl.BlockSpec(shape, lambda i, _: (0,) * len(shape), pipeline_mode=once)
    wide = d + 2 * HEAD
    flops = 2 * tokens * d * (2 * wide + d) + 9 * heads * tokens * tokens * HEAD
    out, keep, send = pl.pallas_call(
        functools.partial(_attend_back_kernel, heads=heads, tokens=tokens),
        name="attend_back",
        grid_spec=pltpu.PrefetchScalarGridSpec(
            num_scalar_prefetch=1,
            grid=(last + 1,),
            in_specs=[rows(d)] * 4 + [whole(tokens, HEAD)] * 2 + [pl.BlockSpec((heads, TILE), lambda i, _: (0, last - i)), rows(HEAD), rows(HEAD)] + [ANY] * 12,
            out_specs=[rows(d), whole(2, d // 4, wide), whole(2, d // 4, wide)],
            scratch_shapes=[pltpu.VMEM((d, wide), BF16), pltpu.VMEM((d, d), BF16), pltpu.VMEM((TILE, d), BF16), pltpu.VMEM((heads, HEAD, TILE), F32),
                            pltpu.VMEM((tokens, HEAD), F32), pltpu.VMEM((tokens, HEAD), F32), pltpu.VMEM((TILE, wide), BF16), pltpu.VMEM((d, TILE), BF16),
                            pltpu.VMEM((d, wide), F32), pltpu.VMEM((8, TILE), F32), pltpu.SemaphoreType.DMA],
        ),
        out_shape=[jax.ShapeDtypeStruct((tokens, d), BF16)] + [jax.ShapeDtypeStruct((2, d // 4, wide), BF16)] * 2,
        compiler_params=pltpu.CompilerParams(dimension_semantics=("arbitrary",), vmem_limit_bytes=VMEM),
        cost_estimate=pl.CostEstimate(flops=flops, transcendentals=heads * tokens * tokens // 2, bytes_accessed=12 * tokens * d),
    )(me, h, dh, q, o, k, v, lse, cos, sin, *wqkv, *wo)
    return out, (keep, send)


def adamw(w, m, v, g):
    m = 0.9 * m + 0.1 * g
    v = 0.95 * v + 0.05 * g * g
    step = m * lax.rsqrt(v + 1e-8) + 0.1 * w
    return (w - 0.02 * step).astype(BF16), m, v


def solution(mesh):
    chip = [(i, i ^ 2) for i in range(4)]
    core = [(i, i ^ 1) for i in range(4)]
    group = [(0, 1), (1, 0)]

    def gathered(w):
        half = w.shape[0] // 2
        px = lax.ppermute(lax.dynamic_slice_in_dim(w, lax.axis_index("rep") * half, half, 0), "dp", chip)
        py = lax.ppermute(px, "rep", group)
        return w, px, py, lax.ppermute(w, "dp", core), lax.ppermute(px, "dp", core), lax.ppermute(py, "dp", core)

    def summed(pair):
        keep, send = pair
        both = keep.astype(F32) + lax.ppermute(send, "dp", core).astype(F32)
        other = lax.ppermute(both[1].astype(BF16), "dp", chip)
        return (both[0] + other.astype(F32)).astype(BF16).astype(F32)

    def step(x, dy, *arrays):
        wq, wk, wv, wo, wg, wu, wd = arrays[:7]
        layers = wq.shape[0]
        me = jnp.stack([lax.axis_index("rep"), lax.axis_index("dp")]).astype(jnp.int32)
        h, tokens = x[0], x.shape[1]
        half = HEAD // 2
        angle = jnp.arange(tokens, dtype=F32)[:, None] * THETA ** (-jnp.arange(half, dtype=F32) / half)
        cos, sin = jnp.cos(angle), jnp.sin(angle)
        cos, sin = jnp.concatenate([cos, cos], -1), jnp.concatenate([-sin, sin], -1)
        full = []
        for n in range(layers):
            full.append((gathered(jnp.concatenate([wq[n], wk[n], wv[n]], -1)), gathered(wo[n]), gathered(jnp.concatenate([wg[n], wu[n]], -1)),
                         gathered(wd[n])))
        kept = []
        for n in range(layers):
            fqkv, fo, fgu, fd = full[n]
            q, k, v, o, lse = attend(me, h, cos, sin, fqkv)
            kept.append([h, None, q, k, v, o, lse])
            if n < layers - 1:
                kept[n][1], h = forward(me, h, o, fo, fgu, fd)
        by_h, mine = dy[0], [None] * layers
        for n in reversed(range(layers)):
            h, h1, q, k, v, o, lse = kept[n]
            fqkv, fo, fgu, fd = full[n]
            by_h, h1, gu, down, out = ff_back(me, h if h1 is None else h1, o, by_h, fo, fgu, fd, h1 is None)
            gu, down, out = summed(gu), summed(down), summed(out)
            by_h, qkv = attend_back(me, h, by_h, q, o, k, v, lse, cos, sin, fqkv, fo)
            mine[n] = (summed(qkv), out, gu, down)
        squares = sum(jnp.sum(g * g) for parts in mine for g in parts)
        for perm, axis in ((core, "dp"), (chip, "dp")):
            squares = squares + lax.ppermute(squares, axis, perm)
        count = 4 * sum(g.size for parts in mine for g in parts)
        factor = jnp.minimum(1.0, 0.5 * lax.rsqrt(squares / count + 1e-30))
        d = wq.shape[2]
        pick = (lambda p: p[0][:, :d], lambda p: p[0][:, d : d + HEAD], lambda p: p[0][:, d + HEAD :], lambda p: p[1], lambda p: p[2][0],
                lambda p: p[2][1], lambda p: p[3])
        new = []
        for i in range(7):
            g = jnp.stack([pick[i](parts) for parts in mine]) * factor
            new.append(adamw(arrays[i].astype(F32), arrays[7 + i], arrays[14 + i], g))
        return tuple(one[which] for which in range(3) for one in new)

    states, cut = P(("rep", "dp"), None, None), P(None, "dp", None)
    return jax.shard_map(
        step,
        mesh=mesh,
        in_specs=(states, states) + (cut,) * 21,
        out_specs=(P("rep", "dp", None),) * 21,
        check_vma=False,
    )
```

```python
import functools

import jax
import jax.numpy as jnp
from jax import lax
from jax.experimental import pallas as pl
from jax.experimental.pallas import tpu as pltpu
from jax.sharding import PartitionSpec as P


NEG = -1e30
HIDDEN = 2 * NEG
LOG2E = 1.4426950408889634
HEAD = 128
THETA = 10000
VMEM = 62 * 2**20
TILE = 512
F32, BF16 = jnp.float32, jnp.bfloat16
ANY = pl.BlockSpec(memory_space=pl.ANY)


def _dot(a, b, ca=1, cb=0):
    return lax.dot_general(a, b, (((ca,), (cb,)), ((), ())), preferred_element_type=F32)


def _scale(h):
    return lax.rsqrt(jnp.mean(h * h, -1, keepdims=True) + 1e-6)


def _norm(h):
    h = h.astype(F32)
    return (h * _scale(h)).astype(BF16)


def _norm_back(h, d):
    h = h.astype(F32)
    r = _scale(h)
    n = h * r
    return r * (d - n * jnp.mean(d * n, -1, keepdims=True))


def _turn(t, cos, sin):
    return t * cos + pltpu.roll(t, HEAD // 2, 1) * sin


def _places(pieces, rows, me):
    rep, dp = me
    n, out = len(pieces) // 2, []
    for j in range(4):
        own, far = pieces[j % 2 * n], pieces[j % 2 * n + 1 : (j % 2 + 1) * n]
        if j < 2 or n == 2:
            out.append([(own if j < 2 else far[0], (dp ^ j) * rows, rows)])
        else:
            out.append([(p, (dp ^ j) * rows + half * (rows // 2), rows // 2) for p, half in zip(far, (rep, 1 - rep))])
    return out


def _copies(pieces, dst, rows, me, sem, at=0, width=None, to=0, blocks=range(4)):
    out = []
    for j in blocks:
        for piece, start, size in _places(pieces, rows, me)[j]:
            src = piece if width is None else piece.at[:, pl.ds(at, width)]
            columns = slice(None) if width is None else pl.ds(to, width)
            out.append(pltpu.make_async_copy(src, dst.at[pl.ds(pl.multiple_of(start, size), size), columns], sem))
    return out


def _split(refs, counts):
    out = []
    for n in counts:
        out.append(refs[:n])
        refs = refs[n:]
    return (*out, refs)


def _attend_kernel(me_ref, h_ref, cos_ref, sin_ref, *rest, tokens, heads, counts):
    w, rest = _split(rest, counts)
    q_ref, k_ref, v_ref, o_ref, lse_ref, w_s, k_s, v_s, top_s, mix_s, sem = rest
    iq = pl.program_id(0)
    d = heads * HEAD
    e = HEAD**-0.5 * LOG2E

    @pl.when(iq == 0)
    def _():
        todo = _copies(w, w_s, w_s.shape[0] // 4, (me_ref[0], me_ref[1]), sem)
        for c in todo:
            c.start()
        for c in todo:
            c.wait()
        v_s[HEAD:, :] = jnp.ones((8, tokens), BF16)

    y = _dot(_norm(h_ref[...]), w_s[...]).astype(BF16)
    cos, sin = cos_ref[...], sin_ref[...]
    for n in range(heads):
        q_ref[:, n * HEAD : (n + 1) * HEAD] = _turn(y[:, n * HEAD : (n + 1) * HEAD].astype(F32), cos, sin).astype(BF16)
    k = _turn(y[:, d : d + HEAD].astype(F32), cos, sin).astype(BF16)
    v = y[:, d + HEAD :]
    k_ref[...] = k
    v_ref[...] = v
    here = pl.ds(pl.multiple_of(iq * TILE, TILE), TILE)
    k_s[here, :] = k
    v_s[:HEAD, here] = v.T
    top_s[...] = jnp.full(top_s.shape, NEG, F32)
    mix_s[...] = jnp.zeros(mix_s.shape, F32)

    def block(start, size, first, masked):
        keys = pl.ds(pl.multiple_of(start, 256), size)
        width = TILE - first
        scores = [_dot(k_s[keys, :], q_ref[first:, n * HEAD : (n + 1) * HEAD], 1, 1) for n in range(heads)]
        if masked:
            ok = lax.broadcasted_iota(jnp.int32, (size, width), 1) >= lax.broadcasted_iota(jnp.int32, (size, width), 0)
        weights, keeps = [], []
        for n, s in enumerate(scores):
            if masked:
                s = jnp.where(ok, s, HIDDEN)
            old = top_s[n : n + 1, first:]
            top = jnp.maximum(old, s.max(axis=0, keepdims=True))
            top_s[n : n + 1, first:] = top
            weights.append(jnp.exp2((s - top) * e).astype(BF16))
            keeps.append(jnp.exp2((old - top) * e))
        for n, (p, keep) in enumerate(zip(weights, keeps)):
            mix_s[n, :, first:] = mix_s[n, :, first:] * keep + _dot(v_s[:, keys], p)

    lax.fori_loop(0, iq, lambda j, _: block(j * TILE, TILE, 0, False), None)
    block(iq * TILE, 256, 0, True)
    block(iq * TILE + 256, 256, 256, True)
    for n in range(heads):
        total = mix_s[n, HEAD : HEAD + 1, :]
        o_ref[:, n * HEAD : (n + 1) * HEAD] = (mix_s[n, :HEAD, :] * (1 / total)).T.astype(BF16)
        lse_ref[n : n + 1, :] = top_s[n : n + 1, :] * e + jnp.log2(total)


def attend(me, h, cos, sin, w):
    tokens, d = h.shape
    heads = d // HEAD
    rows = lambda n: pl.BlockSpec((TILE, n), lambda i, _: (i, 0))
    flops = 2 * tokens * d * (d + 2 * HEAD) + 3 * 2 * heads * tokens * tokens * HEAD
    return pl.pallas_call(
        functools.partial(_attend_kernel, tokens=tokens, heads=heads, counts=(len(w),)),
        name="attend",
        grid_spec=pltpu.PrefetchScalarGridSpec(
            num_scalar_prefetch=1,
            grid=(tokens // TILE,),
            in_specs=[rows(d), rows(HEAD), rows(HEAD)] + [ANY] * len(w),
            out_specs=[rows(d), rows(HEAD), rows(HEAD), rows(d), pl.BlockSpec((heads, TILE), lambda i, _: (0, i))],
            scratch_shapes=[pltpu.VMEM((d, d + 2 * HEAD), BF16), pltpu.VMEM((tokens, HEAD), BF16), pltpu.VMEM((HEAD + 8, tokens), BF16),
                            pltpu.VMEM((8, TILE), F32), pltpu.VMEM((heads, HEAD + 8, TILE), F32), pltpu.SemaphoreType.DMA],
        ),
        out_shape=[jax.ShapeDtypeStruct((tokens, d), BF16), jax.ShapeDtypeStruct((tokens, HEAD), BF16), jax.ShapeDtypeStruct((tokens, HEAD), BF16),
                   jax.ShapeDtypeStruct((tokens, d), BF16), jax.ShapeDtypeStruct((heads, tokens), F32)],
        compiler_params=pltpu.CompilerParams(dimension_semantics=("arbitrary",), vmem_limit_bytes=VMEM),
        cost_estimate=pl.CostEstimate(flops=flops, transcendentals=heads * tokens * tokens // 2, bytes_accessed=10 * tokens * d),
    )(me, h, cos, sin, *w)


def _forward_kernel(me_ref, h_ref, o_ref, *rest, ff, counts):
    wo, wgu, wd, rest = _split(rest, counts)
    h1_ref, h2_ref, wo_s, wg_s, wu_s, wd_s, act_s, sem = rest
    first = pl.program_id(0) == 0
    me = (me_ref[0], me_ref[1])
    d = wo_s.shape[0]
    loads = (lambda: _copies(wo, wo_s, d // 4, me, sem.at[0]),
             lambda: _copies(wgu, wg_s, d // 4, me, sem.at[1], 0, ff) + _copies(wgu, wu_s, d // 4, me, sem.at[1], ff, ff),
             lambda: _copies(wd, wd_s, ff // 4, me, sem.at[2]))

    @pl.when(first)
    def _():
        for group in loads:
            for c in group():
                c.start()
        for c in loads[0]():
            c.wait()

    proj = _dot(o_ref[...], wo_s[...]).astype(BF16)
    h1 = (h_ref[...].astype(F32) + proj.astype(F32)).astype(BF16)
    h1_ref[...] = h1
    b = _norm(h1)

    @pl.when(first)
    def _():
        for group in loads[1:]:
            for c in group():
                c.wait()

    for at in range(0, ff, TILE):
        g = _dot(b, wg_s[:, at : at + TILE])
        u = _dot(b, wu_s[:, at : at + TILE])
        act_s[:, at : at + TILE] = (g * (1 / (1 + jnp.exp(-g))) * u).astype(BF16)
    y = _dot(act_s[...], wd_s[...]).astype(BF16)
    h2_ref[...] = (h1.astype(F32) + y.astype(F32)).astype(BF16)


def forward(me, h, o, wo, wgu, wd):
    tokens, d = h.shape
    ff = wgu[0].shape[1] // 2
    rows = pl.BlockSpec((TILE, d), lambda i, _: (i, 0))
    return pl.pallas_call(
        functools.partial(_forward_kernel, ff=ff, counts=(len(wo), len(wgu), len(wd))),
        name="forward",
        grid_spec=pltpu.PrefetchScalarGridSpec(
            num_scalar_prefetch=1,
            grid=(tokens // TILE,),
            in_specs=[rows, rows] + [ANY] * (len(wo) + len(wgu) + len(wd)),
            out_specs=[rows, rows],
            scratch_shapes=[pltpu.VMEM((d, d), BF16), pltpu.VMEM((d, ff), BF16), pltpu.VMEM((d, ff), BF16), pltpu.VMEM((ff, d), BF16),
                            pltpu.VMEM((TILE, ff), BF16), pltpu.SemaphoreType.DMA((3,))],
        ),
        out_shape=[jax.ShapeDtypeStruct((tokens, d), BF16)] * 2,
        compiler_params=pltpu.CompilerParams(dimension_semantics=("arbitrary",), vmem_limit_bytes=VMEM),
        cost_estimate=pl.CostEstimate(flops=2 * tokens * d * (d + 3 * ff), transcendentals=tokens * ff, bytes_accessed=8 * tokens * d + 2 * d * (d + 3 * ff)),
    )(me, h, o, *wo, *wgu, *wd)


def _ff_back_kernel(me_ref, h_ref, o_ref, dy_ref, *rest, ff, project, counts):
    wo, wgu, wd, rest = _split(rest, counts)
    dh_ref, rest = rest[0], rest[1:]
    h1_ref, rest = (rest[0], rest[1:]) if project else (None, rest)
    gu_keep, gu_send, d_keep, d_send, o_keep, o_send = rest[:6]
    wo_s, rest = (rest[6], rest[7:]) if project else (None, rest[6:])
    wg_s, wu_s, wd_s, h_s, o_s, dy_s, b_s, db_s, act_s, dg_s, du_s, g_s, h_sem, o_sem, w_sem, out_sem = rest
    step = pl.program_id(0)
    me = (me_ref[0], me_ref[1])
    tokens, d = h_s.shape
    rows = d // 4
    tiles = range(0, tokens, TILE)

    def part(src, dst, at, sem):
        here = pl.ds(at, TILE)
        return pltpu.make_async_copy(src.at[here, :], dst.at[here, :], sem)

    def weights(j):
        at = pl.multiple_of((me[1] ^ j) * TILE, TILE)
        out = _copies(wd, wd_s, ff // 4, me, w_sem.at[j], blocks=(j,))
        for base, dst in ((0, wg_s), (ff, wu_s)):
            out += _copies(wgu, dst, rows, me, w_sem.at[j], base + at, TILE, at)
        return out

    h_loads = [part(h_ref, h_s, at, h_sem.at[i]) for i, at in enumerate(tiles)]
    o_loads = [part(o_ref, o_s, at, o_sem.at[i]) for i, at in enumerate(tiles)]

    @pl.when(step == 0)
    def _():
        load_wo = _copies(wo, wo_s, rows, me, out_sem.at[2]) if project else []
        load_dy = pltpu.make_async_copy(dy_ref, dy_s, out_sem.at[3])
        for c in load_wo + h_loads + (o_loads if project else []) + weights(0) + [load_dy] + weights(1) + weights(2) + weights(3) + ([] if project else o_loads):
            c.start()
        for c in load_wo:
            c.wait()
        for i, at in enumerate(tiles):
            here = slice(at, at + TILE)
            h_loads[i].wait()
            h = h_s[here, :]
            if project:
                o_loads[i].wait()
                h = (h.astype(F32) + _dot(o_s[here, :], wo_s[...]).astype(BF16).astype(F32)).astype(BF16)
                h_s[here, :] = h
                part(h_s, h1_ref, at, out_sem.at[0]).start()
            b_s[here, :] = _norm(h)
        db_s[...] = jnp.zeros(db_s.shape, F32)
        load_dy.wait()

    for j in range(4):
        @pl.when(step == j)
        def _():
            for c in weights(j):
                c.wait()

    cols = pl.ds(pl.multiple_of((me[1] ^ step) * TILE, TILE), TILE)
    for at in tiles:
        here = slice(at, at + TILE)
        b = b_s[here, :]
        g = _dot(b, wg_s[:, cols])
        u = _dot(b, wu_s[:, cols])
        da = _dot(dy_s[here, :], wd_s[cols, :], 1, 1).astype(BF16).astype(F32)
        sig = 1 / (1 + jnp.exp(-g))
        silu = g * sig
        act_s[here, :] = (silu * u).astype(BF16)
        dg = (da * u * (sig * (1 + g * (1 - sig)))).astype(BF16)
        du = (da * silu).astype(BF16)
        dg_s[here, :] = dg
        du_s[here, :] = du
        db_s[here, :] += _dot(dg, wg_s[:, cols], 1, 1) + _dot(du, wu_s[:, cols], 1, 1)

    def block(j):
        return pl.ds(pl.multiple_of((me[1] ^ j) * rows, rows), rows)

    for n, grad in enumerate((dg_s, du_s)):
        g_s[:, :TILE] = _dot(b_s[...], grad[...], 0, 0).astype(BF16)
        for j, to in enumerate((gu_keep, gu_send, gu_keep, gu_send)):
            to[j // 2, n] = g_s[block(j), :TILE]
    grad = _dot(act_s[...], dy_s[...], 0, 0).astype(BF16)

    @pl.when(step % 2 == 0)
    def _():
        d_keep[0] = grad

    @pl.when(step % 2 == 1)
    def _():
        d_send[0] = grad

    @pl.when(step == 3)
    def _():
        if not project:
            for c in o_loads:
                c.wait()
        for at in tiles:
            here = slice(at, at + TILE)
            db = db_s[here, :].astype(BF16).astype(F32)
            dy_s[here, :] = (dy_s[here, :].astype(F32) + _norm_back(h_s[here, :], db).astype(BF16).astype(F32)).astype(BF16)
            part(dy_s, dh_ref, at, out_sem.at[1]).start()
        g_s[...] = _dot(o_s[...], dy_s[...], 0, 0).astype(BF16)
        for j, to in enumerate((o_keep, o_send, o_keep, o_send)):
            to[j // 2] = g_s[block(j), :]
        for at in tiles:
            part(dy_s, dh_ref, at, out_sem.at[1]).wait()
            if project:
                part(h_s, h1_ref, at, out_sem.at[0]).wait()


def ff_back(me, h, o, dy, wo, wgu, wd, project):
    tokens, d = h.shape
    ff = wgu[0].shape[1] // 2
    once = pl.Buffered(1)
    whole = lambda *shape: pl.BlockSpec(shape, lambda i, _: (0,) * len(shape), pipeline_mode=once)
    gu = pl.BlockSpec((2, 2, d // 4, TILE), lambda i, me: (0, 0, 0, me[1] ^ i))
    down = pl.BlockSpec((1, TILE, d), lambda i, _: (i // 2, 0, 0))
    states = jax.ShapeDtypeStruct((tokens, d), BF16)
    gu_shape = jax.ShapeDtypeStruct((2, 2, d // 4, ff), BF16)
    down_shape = jax.ShapeDtypeStruct((2, ff // 4, d), BF16)
    o_shape = jax.ShapeDtypeStruct((2, d // 4, d), BF16)
    n_states = 2 if project else 1
    counts = (len(wo) if project else 0, len(wgu), len(wd))
    low = lambda *shape: pltpu.VMEM(shape, BF16)
    out = pl.pallas_call(
        functools.partial(_ff_back_kernel, ff=ff, project=project, counts=counts),
        name="ff_back",
        grid_spec=pltpu.PrefetchScalarGridSpec(
            num_scalar_prefetch=1,
            grid=(4,),
            in_specs=[ANY] * (3 + sum(counts)),
            out_specs=[ANY] * n_states + [gu, gu, down, down, whole(2, d // 4, d), whole(2, d // 4, d)],
            scratch_shapes=([low(d, d)] if project else [])
            + [low(d, ff), low(d, ff), low(ff, d), low(tokens, d), low(tokens, d), low(tokens, d), low(tokens, d), pltpu.VMEM((tokens, d), F32),
               low(tokens, TILE), low(tokens, TILE), low(tokens, TILE), low(d, d), pltpu.SemaphoreType.DMA((4,)), pltpu.SemaphoreType.DMA((4,)),
               pltpu.SemaphoreType.DMA((4,)), pltpu.SemaphoreType.DMA((4,))],
        ),
        out_shape=[states] * n_states + [gu_shape, gu_shape, down_shape, down_shape, o_shape, o_shape],
        compiler_params=pltpu.CompilerParams(dimension_semantics=("arbitrary",), vmem_limit_bytes=VMEM),
        cost_estimate=pl.CostEstimate(flops=2 * tokens * d * (8 * ff + d * n_states), transcendentals=tokens * ff,
                                      bytes_accessed=10 * tokens * d + 12 * d * ff),
    )(me, h, o, dy, *((*wo,) if project else ()), *wgu, *wd)
    dh, h1 = (out[0], out[1]) if project else (out[0], h)
    gu_keep, gu_send, d_keep, d_send, o_keep, o_send = out[n_states:]
    return dh, h1, (gu_keep, gu_send), (d_keep, d_send), (o_keep, o_send)


def _attend_back_kernel(me_ref, h_ref, dh_ref, q_ref, o_ref, k_ref, v_ref, lse_ref, cos_ref, sin_ref, *rest, heads, tokens, counts):
    wqkv, wo, rest = _split(rest, counts)
    out_ref, keep, send, w_s, wo_s, do_s, dq_s, dk_s, dv_s, dqkv_s, a_s, acc_s, delta_s, sem = rest
    step = pl.program_id(0)
    iq = tokens // TILE - 1 - step
    me = (me_ref[0], me_ref[1])
    d = heads * HEAD
    rows = d // 4
    scale = HEAD**-0.5
    e = scale * LOG2E

    @pl.when(step == 0)
    def _():
        todo = _copies(wqkv, w_s, rows, me, sem) + _copies(wo, wo_s, rows, me, sem)
        for c in todo:
            c.start()
        for c in todo:
            c.wait()
        dk_s[...] = jnp.zeros(dk_s.shape, F32)
        dv_s[...] = jnp.zeros(dv_s.shape, F32)
        acc_s[...] = jnp.zeros(acc_s.shape, F32)

    do_s[...] = _dot(dh_ref[...], wo_s[...], 1, 1).astype(BF16)
    for n in range(heads):
        at = slice(n * HEAD, (n + 1) * HEAD)
        delta_s[n : n + 1, :] = (do_s[:, at].astype(F32) * o_ref[:, at].astype(F32)).T.sum(axis=0, keepdims=True)
    dq_s[...] = jnp.zeros(dq_s.shape, F32)

    def block(start, size, first, masked):
        keys = pl.ds(pl.multiple_of(start, 256), size)
        width = TILE - first
        ats = [slice(n * HEAD, (n + 1) * HEAD) for n in range(heads)]
        k, v = k_ref[keys, :], v_ref[keys, :]
        scores = [_dot(k, q_ref[first:, at], 1, 1) for at in ats]
        dps = [_dot(v, do_s[first:, at], 1, 1) for at in ats]
        if masked:
            ok = lax.broadcasted_iota(jnp.int32, (size, width), 1) >= lax.broadcasted_iota(jnp.int32, (size, width), 0)
        for n, at in enumerate(ats):
            p = jnp.exp2(scores[n] * e - lse_ref[n : n + 1, first:])
            if masked:
                p = jnp.where(ok, p, 0.0)
            ds = (p * (dps[n] - delta_s[n : n + 1, first:])).astype(BF16)
            dv_s[keys, :] += _dot(p.astype(BF16), do_s[first:, at])
            dk_s[keys, :] += _dot(ds, q_ref[first:, at])
            dq_s[n, :, first:] += _dot(k.T, ds)

    lax.fori_loop(0, iq, lambda j, _: block(j * TILE, TILE, 0, False), None)
    block(iq * TILE, 256, 0, True)
    block(iq * TILE + 256, 256, 256, True)

    cos, sin = cos_ref[...], -sin_ref[...]
    for n in range(heads):
        dqkv_s[:, n * HEAD : (n + 1) * HEAD] = _turn((dq_s[n] * scale).T.astype(BF16).astype(F32), cos, sin).astype(BF16)
    here = pl.ds(pl.multiple_of(iq * TILE, TILE), TILE)
    dqkv_s[:, d : d + HEAD] = _turn((dk_s[here, :] * scale).astype(BF16).astype(F32), cos, sin).astype(BF16)
    dqkv_s[:, d + HEAD :] = dv_s[here, :].astype(BF16)
    da = _dot(dqkv_s[...], w_s[...], 1, 1).astype(BF16).astype(F32)
    out_ref[...] = (dh_ref[...].astype(F32) + _norm_back(h_ref[...], da).astype(BF16).astype(F32)).astype(BF16)
    a = _norm(h_ref[...])
    for n in range(4):
        to = pl.multiple_of((me[1] ^ n) * rows, rows)
        a_s[pl.ds(to, rows), :] = a[:, n * rows : (n + 1) * rows].T
    acc_s[...] += _dot(a_s[...], dqkv_s[...])

    @pl.when(step == tokens // TILE - 1)
    def _():
        for j, to in enumerate((keep, send, keep, send)):
            to[j // 2] = acc_s[j * rows : (j + 1) * rows, :].astype(BF16)


def attend_back(me, h, dh, q, o, k, v, lse, cos, sin, wqkv, wo):
    tokens, d = h.shape
    heads = d // HEAD
    last = tokens // TILE - 1
    once = pl.Buffered(1)
    rows = lambda n: pl.BlockSpec((TILE, n), lambda i, _: (last - i, 0))
    whole = lambda *shape: pl.BlockSpec(shape, lambda i, _: (0,) * len(shape), pipeline_mode=once)
    wide = d + 2 * HEAD
    flops = 2 * tokens * d * (2 * wide + d) + 9 * heads * tokens * tokens * HEAD
    out, keep, send = pl.pallas_call(
        functools.partial(_attend_back_kernel, heads=heads, tokens=tokens, counts=(len(wqkv), len(wo))),
        name="attend_back",
        grid_spec=pltpu.PrefetchScalarGridSpec(
            num_scalar_prefetch=1,
            grid=(last + 1,),
            in_specs=[rows(d)] * 4 + [whole(tokens, HEAD)] * 2 + [pl.BlockSpec((heads, TILE), lambda i, _: (0, last - i)), rows(HEAD), rows(HEAD)] + [ANY] * (len(wqkv) + len(wo)),
            out_specs=[rows(d), whole(2, d // 4, wide), whole(2, d // 4, wide)],
            scratch_shapes=[pltpu.VMEM((d, wide), BF16), pltpu.VMEM((d, d), BF16), pltpu.VMEM((TILE, d), BF16), pltpu.VMEM((heads, HEAD, TILE), F32),
                            pltpu.VMEM((tokens, HEAD), F32), pltpu.VMEM((tokens, HEAD), F32), pltpu.VMEM((TILE, wide), BF16), pltpu.VMEM((d, TILE), BF16),
                            pltpu.VMEM((d, wide), F32), pltpu.VMEM((8, TILE), F32), pltpu.SemaphoreType.DMA],
        ),
        out_shape=[jax.ShapeDtypeStruct((tokens, d), BF16)] + [jax.ShapeDtypeStruct((2, d // 4, wide), BF16)] * 2,
        compiler_params=pltpu.CompilerParams(dimension_semantics=("arbitrary",), vmem_limit_bytes=VMEM),
        cost_estimate=pl.CostEstimate(flops=flops, transcendentals=heads * tokens * tokens // 2, bytes_accessed=12 * tokens * d),
    )(me, h, dh, q, o, k, v, lse, cos, sin, *wqkv, *wo)
    return out, (keep, send)


def adamw(w, m, v, g):
    m = 0.9 * m + 0.1 * g
    v = 0.95 * v + 0.05 * g * g
    step = m * lax.rsqrt(v + 1e-8) + 0.1 * w
    return (w - 0.02 * step).astype(BF16), m, v


def solution(mesh):
    chip = [(i, i ^ 2) for i in range(4)]
    core = [(i, i ^ 1) for i in range(4)]
    group = [(0, 1), (1, 0)]

    def gathered(w, swap):
        if swap:
            half = w.shape[0] // 2
            px = lax.ppermute(lax.dynamic_slice_in_dim(w, lax.axis_index("rep") * half, half, 0), "dp", chip)
            mine = [w, px, lax.ppermute(px, "rep", group)]
        else:
            mine = [w, lax.ppermute(w, "dp", chip)]
        return (*mine, *(lax.ppermute(p, "dp", core) for p in mine))

    def summed(pair):
        keep, send = pair
        got = lax.ppermute(send, "dp", core)
        far = (keep[1].astype(F32) + got[1].astype(F32)).astype(BF16)
        other = lax.ppermute(far, "dp", chip)
        return (keep[0].astype(F32) + got[0].astype(F32) + other.astype(F32)).astype(BF16).astype(F32)

    def inner(x, dy, *arrays):
        wq, wk, wv, wo, wg, wu, wd = arrays[:7]
        layers = wq.shape[0]
        me = jnp.stack([lax.axis_index("rep"), lax.axis_index("dp")]).astype(jnp.int32)
        h, tokens = x[0], x.shape[1]
        half = HEAD // 2
        angle = jnp.arange(tokens, dtype=F32)[:, None] * THETA ** (-jnp.arange(half, dtype=F32) / half)
        cos, sin = jnp.cos(angle), jnp.sin(angle)
        cos, sin = jnp.concatenate([cos, cos], -1), jnp.concatenate([-sin, sin], -1)
        full = []
        for n in range(layers):
            full.append((gathered(jnp.concatenate([wq[n], wk[n], wv[n]], -1), False), gathered(wo[n], n > 0),
                         gathered(jnp.concatenate([wg[n], wu[n]], -1), n > 0), gathered(wd[n], n > 0)))
        kept = []
        for n in range(layers):
            fqkv, fo, fgu, fd = full[n]
            q, k, v, o, lse = attend(me, h, cos, sin, fqkv)
            kept.append([h, None, q, k, v, o, lse])
            if n < layers - 1:
                kept[n][1], h = forward(me, h, o, fo, fgu, fd)
        by_h, mine = dy[0], [None] * layers
        for n in reversed(range(layers)):
            h, h1, q, k, v, o, lse = kept[n]
            fqkv, fo, fgu, fd = full[n]
            by_h, h1, gu, down, out = ff_back(me, h if h1 is None else h1, o, by_h, fo, fgu, fd, h1 is None)
            gu, down, out = summed(gu), summed(down), summed(out)
            by_h, qkv = attend_back(me, h, by_h, q, o, k, v, lse, cos, sin, fqkv, fo)
            mine[n] = (summed(qkv), out, gu, down)
        squares = sum(jnp.sum(g * g) for parts in mine for g in parts)
        for perm, axis in ((core, "dp"), (chip, "dp")):
            squares = squares + lax.ppermute(squares, axis, perm)
        count = 4 * sum(g.size for parts in mine for g in parts)
        factor = jnp.minimum(1.0, 0.5 * lax.rsqrt(squares / count + 1e-30))
        d = wq.shape[2]
        pick = (lambda p: p[0][:, :d], lambda p: p[0][:, d : d + HEAD], lambda p: p[0][:, d + HEAD :], lambda p: p[1], lambda p: p[2][0],
                lambda p: p[2][1], lambda p: p[3])
        new = []
        for i in range(7):
            g = jnp.stack([pick[i](parts) for parts in mine]) * factor
            new.append(adamw(arrays[i].astype(F32), arrays[7 + i], arrays[14 + i], g))
        return tuple(one[which] for which in range(3) for one in new)

    states, cut = P(("rep", "dp"), None, None), P(None, "dp", None)
    return jax.shard_map(
        inner,
        mesh=mesh,
        in_specs=(states, states) + (cut,) * 21,
        out_specs=(P("rep", "dp", None),) * 21,
        check_vma=False,
    )
```
